32 devices in a mesh: row: 8 (over z, y), col: 4 (over x, core).
Axes of the slice: x: 2, y: 2, z: 4, core: 2. Of those that a mesh axis runs over, the one named last changes fastest.
Arguments:
- grads: float32 [64, 20, 3, 4096], P(None, None, None, ('row', 'col')), may hold values from -6 to 6
- weights: float32 [64, 4096], P(None, ('row', 'col')), may hold values from 0.005 to 0.05
- counts: int32 [4096], P(('row', 'col')), may hold values from 1 to 8
- lame_first: float32 [4096], P(('row', 'col')), may hold values from 0.5 to 2
- shear: float32 [4096], P(('row', 'col')), may hold values from 0.5 to 2
- dest_owner: int32 [4096, 1], P(('row', 'col')), may hold values from 0 to 31; in each aligned block of 128 rows (0 to 127, 128 to 255, ...) at most 8 rows name the same one
- dest_slot: int32 [4096], P(('row', 'col')), may hold values from 0 to 127
Outputs:
- assembled: float32 [60, 60, 4096], P(None, None, ('row', 'col'))
The draws below stay inside these ranges and needn't reach their ends.
Inputs may be any that keep to these rules, and one draw needn't show every extreme that they name: `dest_owner`: among the elements of one device, at most 8 have the same owner; in some device exactly 8 do.
All inputs are finite; a program needn't handle non-finite values.
Results may differ from the reference program's by a relative error of at most 0.0001.
Values sent between devices are 32-bit elements; how exact they have to be, the bound alone decides.
No kernel may reach another device: no remote copies, remote signals or barrier semaphores. Data moves between devices by JAX's collectives and lax.ppermute only.
A program may use at most 64 MiB of HBM per device.

```python
import math
import jax
import jax.numpy as jnp
import numpy as np
from jax import lax

NF = 20
NDOF = 60
GP = 8
SUBMAX = 8
Q = 64
E_DEV = 128
SLOTS_DEV = 128
ELEMS = 4096
SLOTS = 4096
CAP = 8
N_ROW = 8
N_COL = 4
DEVICES = 32


def plant(entries, rng, low, high):
    longest = entries.shape.index(max(entries.shape))
    spots = []
    for shift in (0, 1):
        where = [jax.random.randint(jax.random.fold_in(rng, axis), (), 0, length) for axis, length in enumerate(entries.shape)]
        where[longest] = (where[longest] + shift) % entries.shape[longest]
        spots.append(tuple(where))
    return entries.at[spots[0]].set(low).at[spots[1]].set(high)


def steps_of(stream_key, dims, split, smallest, high):
    def one(position, shards_of):
        draws = jax.random.uniform(jax.random.fold_in(jax.random.fold_in(stream_key, 6), position), (shards_of,), jnp.float32, smallest / len(split), high / len(split))
        return jnp.repeat(jnp.exp(draws), dims[position] // shards_of).reshape((-1,) + (1,) * (len(dims) - position - 1))

    gain = one(*split[0])
    for cut in split[1:]:
        gain = gain * one(*cut)
    return gain


def assign_block(rng, own, number, rows, number_of, top, limit, skew):
    order = jax.random.permutation(rng, number_of)
    crowded, usual = load_shares(number_of, rows * top, limit, skew, True), load_shares(number_of, rows * top, limit, skew, False)
    places = jnp.arange(number_of)

    def named(lengths, turn):
        used = int((lengths > 0).sum())
        fixed = max(1, used // 4)
        moved = fixed + (places - fixed + turn * (used - fixed)) % max(1, number_of - fixed)
        return jnp.zeros((number_of,), jnp.int32).at[order[jnp.where(places < fixed, places, moved)]].set(jnp.asarray(lengths, jnp.int32))

    lengths = jnp.where(number % 4 == 0, named(crowded, number // 4), named(usual, number - number // 4 - 1))
    mixed = jax.random.permutation(jax.random.fold_in(own, 3), number_of)
    giver, sink = mixed[0:number_of // 2 * 2:2], mixed[1:number_of // 2 * 2:2]
    margin = jnp.minimum(lengths[giver] - 1, limit - lengths[sink]) // 2
    margin = jnp.where((giver == order[0]) | (sink == order[0]) | (lengths[sink] == 0), 0, jnp.maximum(margin, 0))
    moved = jax.random.randint(jax.random.fold_in(own, 4), (number_of // 2,), 0, 1 << 20) % (margin + 1)
    lengths = lengths.at[giver].add(-moved).at[sink].add(moved)
    members = jnp.searchsorted(jnp.cumsum(lengths), jnp.arange(rows * top), side="right").astype(jnp.int32)
    listing = members.reshape(top, rows).T
    listing = listing[jax.random.permutation(jax.random.fold_in(own, 1), rows)]
    turn = jax.random.randint(jax.random.fold_in(own, 2), (rows, 1), 0, top)
    return jnp.take_along_axis(listing, (jnp.arange(top)[None, :] + turn) % top, axis=1)


def load_shares(number_of, total, reach, lean, full):
    weights = [(1 << 20) // math.isqrt(rank ** lean) + 1 for rank in range(1, number_of + 1)]
    largest = reach if full else min(reach, max(-(-total // number_of), total * weights[0] // sum(weights)))
    least = 1 if total - largest >= number_of - 1 else 0
    given, surplus = [largest] + [least] * (number_of - 1), total - largest - least * (number_of - 1)
    while surplus > 0:
        free = [i for i in range(1, number_of) if given[i] < largest] or [i for i in range(1, number_of) if given[i] < reach]
        pool, budget = sum([weights[i] for i in free]), surplus
        for i in free:
            addition = min(reach - given[i], max(1, budget * weights[i] // pool), surplus)
            given[i] = given[i] + addition
            surplus = surplus - addition
    return np.array(given)


def normal_values(rng, shape, scale, limit, shards=(), held_as=jnp.bfloat16):
    values = scale * jax.random.normal(rng, shape, jnp.float32)
    if shards:
        values = values * steps_of(rng, shape, shards, -0.22, 0.18)
    return jnp.clip(values, -limit, limit).astype(held_as)


def setup_inputs(seed: int = 0) -> dict:
    key_of = jax.random.split(jax.random.key(seed), 8)
    grads = normal_values(key_of[0], (Q, NF, 3, ELEMS), 1.0, 6.0, ((3, 32),), jnp.float32)
    weights = jnp.clip(jnp.exp(math.log(0.05) - 2.3025851 * jax.random.uniform(key_of[1], (Q, ELEMS), jnp.float32) ** steps_of(key_of[1], (Q, ELEMS), ((1, 32),), -0.2, 0.2)), 0.005, 0.05)
    counts = plant(jax.random.randint(key_of[2], (ELEMS,), 1, SUBMAX + 1), jax.random.fold_in(key_of[2], 1), 1, SUBMAX).astype(jnp.int32)
    lame_first = jnp.clip(jnp.exp(math.log(2.0) - 1.3862944 * jax.random.uniform(key_of[3], (ELEMS,), jnp.float32) ** steps_of(key_of[3], (ELEMS,), ((0, 32),), -0.2, 0.2)), 0.5, 2.0)
    shear = jnp.clip(jnp.exp(math.log(2.0) - 1.3862944 * jax.random.uniform(key_of[4], (ELEMS,), jnp.float32) ** steps_of(key_of[4], (ELEMS,), ((0, 32),), -0.2, 0.2)), 0.5, 2.0)
    dest_owner_keys = jax.random.split(jax.random.fold_in(key_of[5], 1), ELEMS // E_DEV)
    dest_owner_turns = jax.random.permutation(jax.random.fold_in(key_of[5], 3), ELEMS // E_DEV)
    dest_owner = jax.vmap(lambda own, number: assign_block(jax.random.fold_in(key_of[5], 2), own, number, E_DEV, DEVICES, 1, CAP, 2))(dest_owner_keys, dest_owner_turns).reshape((ELEMS, 1))
    dest_slot = plant(jax.random.randint(key_of[6], (ELEMS,), 0, SLOTS_DEV), jax.random.fold_in(key_of[6], 1), 0, SLOTS_DEV - 1).astype(jnp.int32)
    return dict(grads=grads, weights=weights, counts=counts, lame_first=lame_first, shear=shear, dest_owner=dest_owner, dest_slot=dest_slot)


def stiffness(gflat, weff, lame_first, shear):
    count = gflat.shape[2]
    moment = jnp.einsum("qme,qne->mne", gflat * weff[:, None, :], gflat, precision=lax.Precision.HIGHEST)
    blocks = moment.reshape(NF, 3, NF, 3, count)
    across = jnp.einsum("akbke->abe", blocks)
    eye = jnp.eye(3, dtype=jnp.float32)
    result = lame_first * blocks + shear * (eye[None, :, None, :, None] * across[:, None, :, None, :] + jnp.transpose(blocks, (0, 3, 2, 1, 4)))
    return result.reshape(NDOF * NDOF, count)


def reference(grads, weights, counts, lame_first, shear, dest_owner, dest_slot):
    points = lax.broadcasted_iota(jnp.int32, weights.shape, 0)
    weff = jnp.where(points < counts[None, :] * GP, weights, jnp.float32(0.0))
    squares = jnp.sum(grads * grads, axis=(1, 2))
    total = jnp.sum((lame_first + 4.0 * shear) * jnp.sum(weff * squares, axis=0))
    scale = total / (NDOF * ELEMS)
    target = (dest_owner[:, 0] * SLOTS_DEV + dest_slot).astype(jnp.int32)
    gflat = grads.reshape(Q, NDOF, ELEMS)

    def add_block(index, accum):
        start = (index * E_DEV).astype(jnp.int32)
        gpart = lax.dynamic_slice_in_dim(gflat, start, E_DEV, 2)
        wpart = lax.dynamic_slice_in_dim(weff, start, E_DEV, 1)
        lpart = lax.dynamic_slice_in_dim(lame_first, start, E_DEV, 0)
        spart = lax.dynamic_slice_in_dim(shear, start, E_DEV, 0)
        tpart = lax.dynamic_slice_in_dim(target, start, E_DEV, 0)
        return accum.at[:, tpart].add(stiffness(gpart, wpart, lpart, spart))

    accum = lax.fori_loop(0, N_ROW * N_COL, add_block, jnp.zeros((NDOF * NDOF, SLOTS), jnp.float32))
    return (accum / scale).reshape(NDOF, NDOF, SLOTS)
```

```python
import functools

import jax
import jax.numpy as jnp
from jax import lax
from jax.experimental import pallas as pl
from jax.experimental.pallas import tpu as pltpu
from jax.sharding import PartitionSpec as P

NF = 20
NDOF = 60
GP = 8
SLOTS_DEV = 128
LANES = 128
AXES = ("row", "col")

PAIRS = NF * (NF - 1) // 2
PAIRS_UP = -(-PAIRS // 8) * 8
DIAG_UP = -(-NF // 8) * 8
DIAG_BASE = 9 * PAIRS_UP
UPPER = ((0, 0), (0, 1), (0, 2), (1, 1), (1, 2), (2, 2))
SLOT_WORD = DIAG_BASE + 6 * DIAG_UP
TRACE_WORD = SLOT_WORD + 1
WORDS = -(-(TRACE_WORD + 1) // LANES) * LANES


def split(value):
    high = value.astype(jnp.bfloat16)
    low = (value - high.astype(jnp.float32)).astype(jnp.bfloat16)
    return high, low


def pick(onehot, value, dims):
    high, low = split(value)
    dot = functools.partial(
        lax.dot_general, dimension_numbers=(dims, ((), ())), preferred_element_type=jnp.float32
    )
    return dot(onehot, high) + dot(onehot, low)


def fold(parts):
    row = lax.broadcasted_iota(jnp.int32, parts[0].shape, 0)
    for bit in (1, 2, 4):
        keep = (row & bit) == 0
        parts = [
            jnp.where(keep, first, second)
            + pltpu.roll(jnp.where(keep, second, first), 8 - bit, 0)
            for first, second in zip(parts[0::2], parts[1::2])
        ]
    return parts[0]


def element_kernel(
    ndevices,
    capacity,
    g_ref,
    w_ref,
    counts_ref,
    lame_ref,
    shear_ref,
    owner_ref,
    slot_ref,
    out_ref,
    wg_ref,
    k_ref,
):
    points, count = w_ref.shape
    width = ndevices * capacity
    qrow = lax.broadcasted_iota(jnp.int32, (points, count), 0)
    weff = jnp.where(qrow < counts_ref[...] * GP, w_ref[...], 0.0)

    def weigh(m, carry):
        wg_ref[m] = g_ref[m] * weff
        return carry

    lax.fori_loop(0, NDOF, weigh, 0, unroll=4)
    lam = jnp.broadcast_to(lame_ref[...], (8, count))
    mu = jnp.broadcast_to(shear_ref[...], (8, count))
    both = lam + mu

    def products(a, b, wanted):
        sums = {}
        for t in range(points // 8):
            rows = pl.ds(8 * t, 8)
            left = [wg_ref[3 * a + i, rows, :] for i in range(3)]
            right = [g_ref[3 * b + j, rows, :] for j in range(3)]
            for i, j in wanted:
                term = left[i] * right[j]
                sums[i, j] = term if t == 0 else sums[i, j] + term
        return sums

    full = tuple((i, j) for i in range(3) for j in range(3))

    def off_diagonal(group, carry):
        parts = []
        for k in range(8):
            p = group * 8 + k
            d = p // NF
            a = p - d * NF
            b = a + d + 1
            b = jnp.where(b >= NF, b - NF, b)
            parts.append(products(a, b, full))
        m = {ij: fold([part[ij] for part in parts]) for ij in full}
        across = mu * (m[0, 0] + m[1, 1] + m[2, 2])
        for i, j in full:
            value = both * m[i, i] + across if i == j else lam * m[i, j] + mu * m[j, i]
            start = pl.multiple_of((3 * i + j) * PAIRS_UP + group * 8, 8)
            k_ref[pl.ds(start, 8), :] = value
        return carry

    lax.fori_loop(0, PAIRS_UP // 8, off_diagonal, 0)

    row = lax.broadcasted_iota(jnp.int32, (8, count), 0)

    def diagonal(group, trace):
        parts = []
        for k in range(8):
            a = jnp.minimum(group * 8 + k, NF - 1)
            parts.append(products(a, a, UPPER))
        m = {ij: fold([part[ij] for part in parts]) for ij in UPPER}
        inside = m[0, 0] + m[1, 1] + m[2, 2]
        across = mu * inside
        for c, (i, j) in enumerate(UPPER):
            value = both * m[i, j] + across if i == j else both * m[i, j]
            start = pl.multiple_of(DIAG_BASE + c * DIAG_UP + group * 8, 8)
            k_ref[pl.ds(start, 8), :] = value
        return trace + jnp.where(row + group * 8 < NF, inside, 0.0)

    trace = lax.fori_loop(0, DIAG_UP // 8, diagonal, jnp.zeros((8, count), jnp.float32))
    local = jnp.sum((lam + 4.0 * mu) * trace)

    tail = lax.broadcasted_iota(jnp.int32, (WORDS - SLOT_WORD, count), 0)
    slots = slot_ref[...].astype(jnp.float32) + 1.0
    k_ref[SLOT_WORD:, :] = jnp.where(tail == 0, slots, 0.0)

    owners = lax.broadcasted_iota(jnp.int32, (ndevices, count), 0)
    mine = owner_ref[...] == owners
    onehot = mine.astype(jnp.bfloat16)
    before = (
        lax.broadcasted_iota(jnp.int32, (count, count), 0)
        < lax.broadcasted_iota(jnp.int32, (count, count), 1)
    ).astype(jnp.bfloat16)
    rank = jnp.dot(onehot, before, preferred_element_type=jnp.float32)
    place = jnp.sum(
        jnp.where(mine, owners * capacity + rank.astype(jnp.int32), 0), axis=0, keepdims=True
    )
    send = (lax.broadcasted_iota(jnp.int32, (width, count), 0) == place).astype(jnp.bfloat16)
    lane = lax.broadcasted_iota(jnp.int32, (width, LANES), 1)
    for tile in range(WORDS // LANES):
        words = slice(tile * LANES, (tile + 1) * LANES)
        moved = pick(send, k_ref[words, :], ((1,), (1,)))
        if tile == TRACE_WORD // LANES:
            moved = jnp.where(lane == TRACE_WORD % LANES, local, moved)
        out_ref[:, words] = moved


def owner_kernel(capacity, elements, in_ref, out_ref, sum_ref):
    width = in_ref.shape[0]
    tail = in_ref[:, WORDS - LANES :].T
    slots = tail[SLOT_WORD % LANES : SLOT_WORD % LANES + 1, :]
    traces = tail[TRACE_WORD % LANES : TRACE_WORD % LANES + 1, :]
    total = jnp.sum(traces) / capacity
    inverse = 1.0 / jnp.broadcast_to(total / (NDOF * elements), (SLOTS_DEV, LANES))
    wanted = (lax.broadcasted_iota(jnp.int32, (SLOTS_DEV, width), 0) + 1).astype(jnp.float32)
    placing = (slots == wanted).astype(jnp.bfloat16)
    for tile in range(WORDS // LANES):
        words = slice(tile * LANES, (tile + 1) * LANES)
        summed = pick(placing, in_ref[:, words], ((1,), (0,)))
        sum_ref[words, :] = (summed * inverse).T

    for a in range(NF):
        forth = NF // 2 if a < NF // 2 else NF // 2 - 1
        back = NF - 1 - forth
        runs = []
        near = min(forth, NF - 1 - a)
        runs.append((a + 1, a, NF, near, False))
        runs.append((0, (near) * NF + a, NF, forth - near, False))
        low = min(back, a)
        runs.append((a - low, None, low, low, True))
        runs.append((NF - (back - low), None, back, back - low, True))
        for i in range(3):
            m = 3 * a + i
            for j in range(3):
                for run in runs[:2]:
                    b, word, step, length, _ = run
                    if length:
                        out_ref[m, pl.ds(3 * b + j, length, stride=3), :] = sum_ref[
                            pl.ds((3 * i + j) * PAIRS_UP + word, length, stride=step), :
                        ]
                for b0, _, dmax, length, _ in runs[2:]:
                    for s in range(length):
                        d = dmax - s
                        b = (a - d) % NF
                        word = (3 * j + i) * PAIRS_UP + (d - 1) * NF + b
                        out_ref[m, 3 * b + j, :] = sum_ref[word, :]
                c = UPPER.index((min(i, j), max(i, j)))
                out_ref[m, 3 * a + j, :] = sum_ref[DIAG_BASE + c * DIAG_UP + a, :]


def shards(grads, weights, counts, lame_first, shear, dest_owner, dest_slot):
    points, _, _, count = grads.shape
    ndevices = lax.axis_size("row") * lax.axis_size("col")
    capacity = max(2, 2 * count // ndevices)
    width = ndevices * capacity
    g = jnp.transpose(grads, (1, 2, 0, 3)).reshape(NDOF, points, count)
    line = lambda v: v.reshape(1, count)
    payload = pl.pallas_call(
        functools.partial(element_kernel, ndevices, capacity),
        out_shape=jax.ShapeDtypeStruct((width, WORDS), jnp.float32),
        scratch_shapes=[
            pltpu.VMEM((NDOF, points, count), jnp.float32),
            pltpu.VMEM((WORDS, count), jnp.float32),
        ],
        name="elements",
    )(
        g,
        weights,
        line(counts),
        line(lame_first),
        line(shear),
        line(dest_owner),
        line(dest_slot),
    )
    moved = lax.all_to_all(
        payload.reshape(ndevices, capacity, WORDS), AXES, split_axis=0, concat_axis=0, tiled=True
    )
    return pl.pallas_call(
        functools.partial(owner_kernel, capacity, count * ndevices),
        out_shape=jax.ShapeDtypeStruct((NDOF, NDOF, SLOTS_DEV), jnp.float32),
        scratch_shapes=[pltpu.VMEM((WORDS, SLOTS_DEV), jnp.float32)],
        name="owners",
    )(moved.reshape(width, WORDS))


def solution(mesh):
    in_specs = (
        P(None, None, None, AXES),
        P(None, AXES),
        P(AXES),
        P(AXES),
        P(AXES),
        P(AXES, None),
        P(AXES),
    )
    out_specs = P(None, None, AXES)
    return jax.shard_map(shards, mesh=mesh, in_specs=in_specs, out_specs=out_specs, check_vma=False)
```

```python
import functools

import jax
import jax.numpy as jnp
from jax import lax
from jax.experimental import pallas as pl
from jax.experimental.pallas import tpu as pltpu
from jax.sharding import PartitionSpec as P


NF = 20
NDOF = 60
GP = 8
SLOTS_DEV = 128
LANES = 128
STRIPES = 4
AXES = ("row", "col")

FULL = tuple((i, j) for i in range(3) for j in range(3))
UPPER = ((0, 0), (0, 1), (0, 2), (1, 1), (1, 2), (2, 2))
DIAG_UP = -(-NF // 8) * 8


class Part:
    def __init__(self, first, last, inner, leads):
        self.first, self.last, self.inner, self.leads = first, last, inner, leads
        pairs = sum(NF // 2 if 2 * d == NF else NF for d in range(first, last + 1))
        self.pairs = -(-pairs // 8) * 8
        self.diagonal = 9 * self.pairs
        self.used = self.diagonal + len(inner) * DIAG_UP
        self.slot = self.diagonal + NF if inner else self.used
        self.trace = self.slot + 1
        self.words = -(-(self.used + 2 * leads) // LANES) * LANES


LEAD = Part(1, 4, (), True)
REST = Part(5, 10, UPPER, False)


def split(value):
    high = value.astype(jnp.bfloat16)
    low = (value - high.astype(jnp.float32)).astype(jnp.bfloat16)
    return high, low


def pick(onehot, value, dims):
    high, low = split(value)
    dot = functools.partial(
        lax.dot_general, dimension_numbers=(dims, ((), ())), preferred_element_type=jnp.float32
    )
    return dot(onehot, high) + dot(onehot, low)


def fold(parts):
    row = lax.broadcasted_iota(jnp.int32, parts[0].shape, 0)
    for bit in (1, 2, 4):
        keep = (row & bit) == 0
        parts = [
            jnp.where(keep, first, second)
            + pltpu.roll(jnp.where(keep, second, first), 8 - bit, 0)
            for first, second in zip(parts[0::2], parts[1::2])
        ]
    return parts[0]


def lead_elements(plane, ndevices, capacity, *refs):
    g_hbm, w_hbm, counts_hbm, lame_hbm, shear_hbm, slot_hbm, owner_hbm = refs[:7]
    *out_refs, place_ref, g_ref, wg_ref, lines_ref = refs[7:-8]
    w_ref, counts_ref, lame_ref, shear_ref, slot_ref, owner_ref, k_ref, sems = refs[-8:]
    points, count = w_ref.shape
    width = ndevices * capacity
    small = [
        pltpu.make_async_copy(source, target, sems.at[n])
        for n, (source, target) in enumerate(
            (
                (w_hbm, w_ref),
                (counts_hbm, counts_ref),
                (lame_hbm, lame_ref),
                (shear_hbm, shear_ref),
                (slot_hbm, slot_ref),
                (owner_hbm, owner_ref),
            )
        )
    ]
    stripe = NDOF // STRIPES
    large = [
        pltpu.make_async_copy(
            g_hbm.at[pl.ds(n * stripe, stripe)],
            g_ref.at[pl.ds(n * stripe, stripe)],
            sems.at[len(small) + n],
        )
        for n in range(STRIPES)
    ]
    for copy in small + large:
        copy.start()
    for copy in small:
        copy.wait()

    owners = lax.broadcasted_iota(jnp.int32, (ndevices, count), 0)
    mine = owner_ref[...] == owners
    before = (
        lax.broadcasted_iota(jnp.int32, (count, count), 0)
        < lax.broadcasted_iota(jnp.int32, (count, count), 1)
    ).astype(jnp.bfloat16)
    rank = jnp.dot(
        mine.astype(jnp.bfloat16), before, preferred_element_type=jnp.float32
    ).astype(jnp.int32)

    def place(base):
        return jnp.sum(jnp.where(mine, base * capacity + rank, 0), axis=0, keepdims=True)

    place_ref[...] = place(owners)
    me = lax.axis_index("row") * lax.axis_size("col") + lax.axis_index("col")
    ahead = owners // plane - me // plane
    ahead = jnp.where(ahead < 0, ahead + ndevices // plane, ahead)
    aside = owners % plane - me % plane
    aside = jnp.where(aside < 0, aside + plane, aside)
    where = place(ahead * plane + aside)

    qrow = lax.broadcasted_iota(jnp.int32, (points, count), 0)
    weff = jnp.where(qrow < counts_ref[...] * GP, w_ref[...], 0.0)

    def weigh(m, inside):
        g = g_ref[m]
        weighted = g * weff
        wg_ref[m] = weighted
        return inside + jnp.sum((weighted * g).reshape(points // 8, 8, count), axis=0)

    inside = jnp.zeros((8, count), jnp.float32)
    for n, copy in enumerate(large):
        copy.wait()
        inside = lax.fori_loop(n * stripe, (n + 1) * stripe, weigh, inside, unroll=3)
    slots = slot_ref[...].astype(jnp.float32) + 1.0
    row = lax.broadcasted_iota(jnp.int32, (8, count), 0)
    lam = jnp.broadcast_to(lame_ref[...], (8, count))
    mu = jnp.broadcast_to(shear_ref[...], (8, count))
    lines_ref[...] = jnp.where(row == 0, lam, jnp.where(row == 1, mu, slots))
    local = jnp.sum((lam + 4.0 * mu) * inside)
    blocks(LEAD, g_ref, wg_ref, lam, mu, slots[:1], k_ref)

    lane = lax.broadcasted_iota(jnp.int32, (width, LANES), 1)
    rows = plane * capacity
    for words, moved in selected(LEAD, where, width, k_ref):
        if words.start == LEAD.trace // LANES * LANES:
            moved = jnp.where(lane == LEAD.trace % LANES, local, moved)
        for k, out_ref in enumerate(out_refs):
            out_ref[:, words] = moved[k * rows : (k + 1) * rows]


def rest_elements(g_ref, wg_ref, lines_ref, place_ref, out_ref, k_ref):
    lam, mu, slots = (jnp.broadcast_to(lines_ref[n : n + 1, :], (8, k_ref.shape[1])) for n in range(3))
    blocks(REST, g_ref, wg_ref, lam, mu, slots[:1], k_ref)
    for words, moved in selected(REST, place_ref[...], out_ref.shape[0], k_ref):
        out_ref[:, words] = moved


def selected(part, where, width, k_ref):
    send = (lax.broadcasted_iota(jnp.int32, (width, k_ref.shape[1]), 0) == where).astype(
        jnp.bfloat16
    )
    for tile in range(part.words // LANES):
        words = slice(tile * LANES, (tile + 1) * LANES)
        yield words, pick(send, k_ref[words, :], ((1,), (1,)))


def blocks(part, g_ref, wg_ref, lam, mu, slots, k_ref):
    points, count = g_ref.shape[1:]
    both = lam + mu

    def products(a, b, wanted):
        sums = {}
        for t in range(points // 8):
            rows = pl.ds(8 * t, 8)
            left = [wg_ref[3 * a + i, rows, :] for i in range(3)]
            right = [g_ref[3 * b + j, rows, :] for j in range(3)]
            for i, j in wanted:
                term = left[i] * right[j]
                sums[i, j] = term if t == 0 else sums[i, j] + term
        return sums

    def off_diagonal(group, carry):
        sums = []
        for k in range(8):
            p = group * 8 + k
            d = p // NF
            a = p - d * NF
            b = a + d + part.first
            b = jnp.where(b >= NF, b - NF, b)
            sums.append(products(a, b, FULL))
        m = {ij: fold([one[ij] for one in sums]) for ij in FULL}
        across = mu * (m[0, 0] + m[1, 1] + m[2, 2])
        for i, j in FULL:
            value = both * m[i, i] + across if i == j else lam * m[i, j] + mu * m[j, i]
            start = pl.multiple_of((3 * i + j) * part.pairs + group * 8, 8)
            k_ref[pl.ds(start, 8), :] = value
        return carry

    lax.fori_loop(0, part.pairs // 8, off_diagonal, 0)

    def diagonal(group, carry):
        sums = []
        for k in range(8):
            a = jnp.minimum(group * 8 + k, NF - 1)
            sums.append(products(a, a, part.inner))
        m = {ij: fold([one[ij] for one in sums]) for ij in part.inner}
        if (0, 0) in part.inner:
            across = mu * (m[0, 0] + m[1, 1] + m[2, 2])
        for c, (i, j) in enumerate(part.inner):
            value = both * m[i, j] + across if i == j else both * m[i, j]
            start = pl.multiple_of(part.diagonal + c * DIAG_UP + group * 8, 8)
            k_ref[pl.ds(start, 8), :] = value
        return carry

    if part.inner:
        lax.fori_loop(0, DIAG_UP // 8, diagonal, 0)

    if part.used < part.words:
        k_ref[pl.ds(part.used, part.words - part.used), :] = jnp.zeros(
            (part.words - part.used, count), jnp.float32
        )
    k_ref[pl.ds(part.slot, 1), :] = slots


def gather_words(part, inverse, in_ref, sum_ref):
    width = in_ref.shape[0]
    base = part.slot // LANES * LANES
    tail = in_ref[:, base : base + LANES].T
    slots = tail[part.slot - base : part.slot - base + 1, :]
    wanted = (lax.broadcasted_iota(jnp.int32, (SLOTS_DEV, width), 0) + 1).astype(jnp.float32)
    placing = (slots == wanted).astype(jnp.bfloat16)
    for tile in range(part.words // LANES):
        words = slice(tile * LANES, (tile + 1) * LANES)
        summed = pick(placing, in_ref[:, words], ((1,), (0,)))
        sum_ref[words, :] = (summed * inverse).T


def relay_kernel(plane, capacity, *refs):
    planes = len(refs) - plane
    in_refs, out_refs = refs[:planes], refs[planes:]
    for l, out_ref in enumerate(out_refs):
        for k, in_ref in enumerate(in_refs):
            out_ref[k * capacity : (k + 1) * capacity] = in_ref[l * capacity : (l + 1) * capacity]


def lead_kernel(part, capacity, elements, *refs):
    in_refs, (sum_ref, inverse_ref, all_ref) = refs[:-3], refs[-3:]
    rows = in_refs[0].shape[0]
    for l, in_ref in enumerate(in_refs):
        all_ref[l * rows : (l + 1) * rows] = in_ref[...]
    total = jnp.sum(all_ref[:, part.trace : part.trace + 1]) / capacity
    inverse = 1.0 / jnp.broadcast_to(total / (NDOF * elements), (SLOTS_DEV, LANES))
    inverse_ref[...] = inverse
    gather_words(part, inverse, all_ref, sum_ref)


def last_kernel(in_ref, inverse_ref, lead_ref, out_ref, sum_ref, whole_ref, sems):
    gather_words(REST, inverse_ref[...], in_ref, sum_ref)
    sums = {LEAD: lead_ref, REST: sum_ref}

    def copy(stripe):
        rows = pl.ds(stripe * (NDOF // STRIPES), NDOF // STRIPES)
        return pltpu.make_async_copy(whole_ref.at[rows], out_ref.at[rows], sems.at[stripe])

    for a in range(NF):
        forth = NF // 2 if a < NF // 2 else NF // 2 - 1
        back = NF - 1 - forth
        for i in range(3):
            m = 3 * a + i
            for j in range(3):
                for one, ref in sums.items():
                    for d in range(one.first, one.last + 1):
                        start = (d - one.first) * NF
                        if d <= forth:
                            b = (a + d) % NF
                            word = (3 * i + j) * one.pairs + start + a
                            whole_ref[m, 3 * b + j, :] = ref[word, :]
                        if d <= back:
                            b = (a - d) % NF
                            word = (3 * j + i) * one.pairs + start + b
                            whole_ref[m, 3 * b + j, :] = ref[word, :]
                    ij = (min(i, j), max(i, j))
                    if ij in one.inner:
                        word = one.diagonal + one.inner.index(ij) * DIAG_UP + a
                        whole_ref[m, 3 * a + j, :] = ref[word, :]
        if (a + 1) * STRIPES % NF == 0:
            copy((a + 1) * STRIPES // NF - 1).start()
    for stripe in range(STRIPES):
        copy(stripe).wait()


def shards(grads, weights, counts, lame_first, shear, dest_owner, dest_slot):
    points, _, _, count = grads.shape
    nrow, ncol = lax.axis_size("row"), lax.axis_size("col")
    ndevices = nrow * ncol
    capacity = max(2, 2 * count // ndevices)
    width = ndevices * capacity
    planes = nrow // 2 if nrow % 2 == 0 else nrow
    plane = ndevices // planes
    f32 = lambda *shape: jax.ShapeDtypeStruct(shape, jnp.float32)
    line = lambda v: v.reshape(1, count)
    params = pltpu.CompilerParams(vmem_limit_bytes=20 * 2**20)
    vmem = pltpu.VMEM
    hbm = pl.BlockSpec(memory_space=pltpu.MemorySpace.HBM)
    large = (NDOF, points, count)

    near = lambda d, k: (d + k * plane) % ndevices
    beside = lambda d, l: d // plane * plane + (d + l) % plane
    cost = lambda part: pl.CostEstimate(
        flops=60000 * part.words, bytes_accessed=4000000, transcendentals=0
    )
    *blocks, place, g, wg, lines = pl.pallas_call(
        functools.partial(lead_elements, plane, ndevices, capacity),
        in_specs=[hbm] * 7,
        out_shape=[f32(plane * capacity, LEAD.words)] * planes
        + [jax.ShapeDtypeStruct((1, count), jnp.int32), f32(*large), f32(*large), f32(8, count)],
        scratch_shapes=[
            vmem((points, count), jnp.float32),
            vmem((1, count), jnp.int32),
            vmem((1, count), jnp.float32),
            vmem((1, count), jnp.float32),
            vmem((1, count), jnp.int32),
            vmem((1, count), jnp.int32),
            vmem((LEAD.words, count), jnp.float32),
            pltpu.SemaphoreType.DMA((6 + STRIPES,)),
        ],
        compiler_params=params,
        cost_estimate=cost(LEAD),
        name="elements_lead",
    )(
        *(
            pltpu.with_memory_space_constraint(v, pltpu.MemorySpace.HBM)
            for v in (
                jnp.transpose(grads, (1, 2, 0, 3)).reshape(large),
                weights,
                line(counts),
                line(lame_first),
                line(shear),
                line(dest_slot),
                line(dest_owner),
            )
        )
    )
    for k in range(1, planes):
        pairs = [(d, near(d, k)) for d in range(ndevices)]
        blocks[k] = lax.ppermute(blocks[k], AXES, pairs)
    rest = pl.pallas_call(
        rest_elements,
        out_shape=f32(width, REST.words),
        scratch_shapes=[vmem((REST.words, count), jnp.float32)],
        compiler_params=params,
        cost_estimate=cost(REST),
        name="elements_rest",
    )(g, wg, lines, place)
    rest = lax.all_to_all(
        rest.reshape(ndevices, capacity, REST.words),
        AXES,
        split_axis=0,
        concat_axis=0,
        tiled=True,
    ).reshape(width, REST.words)
    blocks = pl.pallas_call(
        functools.partial(relay_kernel, plane, capacity),
        out_shape=[f32(planes * capacity, LEAD.words)] * plane,
        compiler_params=params,
        name="relay",
    )(*blocks)
    blocks = list(blocks)
    for l in range(1, plane):
        pairs = [(d, beside(d, l)) for d in range(ndevices)]
        blocks[l] = lax.ppermute(blocks[l], AXES, pairs)
    lead, inverse = pl.pallas_call(
        functools.partial(lead_kernel, LEAD, capacity, count * ndevices),
        out_shape=[f32(LEAD.words, SLOTS_DEV), f32(SLOTS_DEV, LANES)],
        scratch_shapes=[pltpu.VMEM((width, LEAD.words), jnp.float32)],
        compiler_params=params,
        name="owners_lead",
    )(*blocks)
    return pl.pallas_call(
        last_kernel,
        out_shape=f32(NDOF, NDOF, SLOTS_DEV),
        out_specs=pl.BlockSpec(memory_space=pl.ANY),
        scratch_shapes=[
            pltpu.VMEM((REST.words, SLOTS_DEV), jnp.float32),
            pltpu.VMEM((NDOF, NDOF, SLOTS_DEV), jnp.float32),
            pltpu.SemaphoreType.DMA((STRIPES,)),
        ],
        compiler_params=params,
        name="owners_last",
    )(rest, inverse, lead)


def solution(mesh):
    in_specs = (
        P(None, None, None, AXES),
        P(None, AXES),
        P(AXES),
        P(AXES),
        P(AXES),
        P(AXES, None),
        P(AXES),
    )
    out_specs = P(None, None, AXES)

    return jax.shard_map(shards, mesh=mesh, in_specs=in_specs, out_specs=out_specs, check_vma=False)
```

```python
import functools

import jax
import jax.numpy as jnp
from jax import lax
from jax.experimental import pallas as pl
from jax.experimental.pallas import tpu as pltpu
from jax.sharding import PartitionSpec as P


NF = 20
NDOF = 60
GP = 8
SLOTS_DEV = 128
LANES = 128
STRIPES = 4
HOPS = lambda planes: range(1, planes)
AXES = ("row", "col")

FULL = tuple((i, j) for i in range(3) for j in range(3))
UPPER = ((0, 0), (0, 1), (0, 2), (1, 1), (1, 2), (2, 2))
DIAG_UP = -(-NF // 8) * 8


def near_pairs(offset):
    def double(t):
        a, d = t % NF, offset + t // NF * 2
        return a, (a + d) % NF, (a + d + 1) % NF

    return double


def far_pairs(t):
    v = lambda k: 9 * k % NF
    m = t // 2 * 4 + 2 + t % 2
    c = (t - NF // 2) * 4 + 1
    mixed = (v(m), v(m + 1), (v(m) + NF // 2) % NF)
    alike = (v(c), v(c + NF - 1), v(c + 1))
    if isinstance(t, int):
        return mixed if t < NF // 2 else alike
    return tuple(jnp.where(t < NF // 2, x, y) for x, y in zip(mixed, alike))


class Part:
    def __init__(self, runs, inner, leads):
        self.runs, self.inner, self.leads = runs, inner, leads
        doubles = [double(t) for double, count in runs for t in range(count)]
        self.blocks = [(a, b) for a, *both in doubles for b in both]
        self.pairs = len(self.blocks)
        self.diagonal = 9 * self.pairs
        self.used = self.diagonal + len(inner) * DIAG_UP
        self.slot = self.diagonal + NF if inner else self.used
        self.trace = self.slot + 1
        self.words = -(-(self.used + (0 if inner else 2)) // LANES) * LANES


LEAD = Part(((near_pairs(1), 2 * NF),), (), True)
REST = Part(((near_pairs(5), 2 * NF), (far_pairs, 16)), UPPER, False)
assert {frozenset(pair) for part in (LEAD, REST) for pair in part.blocks} == {
    frozenset((a, b)) for b in range(NF) for a in range(b)
}


def split(value):
    high = value.astype(jnp.bfloat16)
    low = (value - high.astype(jnp.float32)).astype(jnp.bfloat16)
    return high, low


def pick(onehot, value, dims):
    high, low = split(value)
    dot = functools.partial(
        lax.dot_general, dimension_numbers=(dims, ((), ())), preferred_element_type=jnp.float32
    )
    return dot(onehot, high) + dot(onehot, low)


def merge(left, right, bit):
    keep = (lax.broadcasted_iota(jnp.int32, next(iter(left.values())).shape, 0) & bit) == 0
    return {
        key: jnp.where(keep, one, right[key])
        + pltpu.roll(jnp.where(keep, right[key], one), 8 - bit, 0)
        for key, one in left.items()
    }


def octet(two):
    halves = []
    for half in range(2):
        quarters = [merge(*two(2 * half + quarter), 1) for quarter in range(2)]
        halves.append(merge(*quarters, 2))
    return merge(*halves, 4)


def lead_elements(plane, ndevices, capacity, *refs):
    g_hbm, w_hbm, counts_hbm, lame_hbm, shear_hbm, slot_hbm, owner_hbm = refs[:7]
    *out_refs, place_ref, g_ref, wg_ref, lines_ref = refs[7:-8]
    w_ref, counts_ref, lame_ref, shear_ref, slot_ref, owner_ref, k_ref, sems = refs[-8:]
    points, count = w_ref.shape
    width = ndevices * capacity
    small = [
        pltpu.make_async_copy(source, target, sems.at[n])
        for n, (source, target) in enumerate(
            (
                (w_hbm, w_ref),
                (counts_hbm, counts_ref),
                (lame_hbm, lame_ref),
                (shear_hbm, shear_ref),
                (slot_hbm, slot_ref),
                (owner_hbm, owner_ref),
            )
        )
    ]
    stripe = NDOF // STRIPES
    large = [
        pltpu.make_async_copy(
            g_hbm.at[pl.ds(n * stripe, stripe)],
            g_ref.at[pl.ds(n * stripe, stripe), pl.ds(0, points)],
            sems.at[len(small) + n],
        )
        for n in range(STRIPES)
    ]
    for copy in small + large:
        copy.start()
    for copy in small:
        copy.wait()

    owners = lax.broadcasted_iota(jnp.int32, (ndevices, count), 0)
    mine = owner_ref[...] == owners
    before = (
        lax.broadcasted_iota(jnp.int32, (count, count), 0)
        < lax.broadcasted_iota(jnp.int32, (count, count), 1)
    ).astype(jnp.bfloat16)
    rank = jnp.dot(
        mine.astype(jnp.bfloat16), before, preferred_element_type=jnp.float32
    ).astype(jnp.int32)

    def place(base):
        return jnp.sum(jnp.where(mine, base * capacity + rank, 0), axis=0, keepdims=True)

    place_ref[...] = place(owners)
    me = lax.axis_index("row") * lax.axis_size("col") + lax.axis_index("col")
    ahead = (owners // plane) ^ (me // plane)
    aside = owners % plane - me % plane
    aside = jnp.where(aside < 0, aside + plane, aside)
    where = place(ahead * plane + aside)

    qrow = lax.broadcasted_iota(jnp.int32, (points, count), 0)
    weff = jnp.where(qrow < counts_ref[...] * GP, w_ref[...], 0.0)

    def weigh(m, inside):
        g = g_ref[m, :points]
        weighted = g * weff
        wg_ref[m, :points] = weighted
        return inside + jnp.sum((weighted * g).reshape(points // 8, 8, count), axis=0)

    inside = jnp.zeros((8, count), jnp.float32)
    for n, copy in enumerate(large):
        copy.wait()
        inside = lax.fori_loop(n * stripe, (n + 1) * stripe, weigh, inside, unroll=3)
    slots = slot_ref[...].astype(jnp.float32) + 1.0
    row = lax.broadcasted_iota(jnp.int32, (8, count), 0)
    lam = jnp.broadcast_to(lame_ref[...], (8, count))
    mu = jnp.broadcast_to(shear_ref[...], (8, count))
    lines_ref[...] = jnp.where(row == 0, lam, jnp.where(row == 1, mu, slots))
    local = jnp.sum((lam + 4.0 * mu) * inside)
    blocks(LEAD, g_ref, wg_ref, lam, mu, slots[:1], k_ref)

    lane = lax.broadcasted_iota(jnp.int32, (width, LANES), 1)
    rows = plane * capacity
    for words, moved in selected(LEAD, where, width, k_ref):
        if words.start == LEAD.trace // LANES * LANES:
            moved = jnp.where(lane == LEAD.trace % LANES, local, moved)
        for k, out_ref in enumerate(out_refs):
            out_ref[:, words] = moved[k * rows : (k + 1) * rows]


def rest_elements(g_ref, wg_ref, lines_ref, place_ref, out_hbm, k_ref, out_ref, sems):
    lam, mu, slots = (
        jnp.broadcast_to(lines_ref[n : n + 1, :], (8, k_ref.shape[1])) for n in range(3)
    )
    blocks(REST, g_ref, wg_ref, lam, mu, slots[:1], k_ref)
    copies = []
    for words, moved in selected(REST, place_ref[...], out_ref.shape[0], k_ref):
        out_ref[:, words] = moved
        n = len(copies)
        if words.stop % (2 * LANES) == 0 or words.stop == REST.words:
            done = pl.ds(n * 2 * LANES, words.stop - n * 2 * LANES)
            copies.append(
                pltpu.make_async_copy(out_ref.at[:, done], out_hbm.at[:, done], sems.at[n])
            )
            copies[-1].start()
    for copy in copies:
        copy.wait()


def selected(part, where, width, k_ref):
    send = (lax.broadcasted_iota(jnp.int32, (width, k_ref.shape[1]), 0) == where).astype(
        jnp.bfloat16
    )
    for tile in range(part.words // LANES):
        words = slice(tile * LANES, (tile + 1) * LANES)
        yield words, pick(send, k_ref[words, :], ((1,), (1,)))


def blocks(part, g_ref, wg_ref, lam, mu, slots, k_ref):
    points, count = g_ref.shape[1] - 8, g_ref.shape[2]
    both = lam + mu

    def products(a, seconds, wanted):
        sums = [{} for _ in seconds]
        for t in range(points // 8):
            rows = pl.ds(8 * t, 8)
            left = [wg_ref[3 * a + i, rows, :] for i in range(3)]
            for one, b in zip(sums, seconds):
                right = [g_ref[3 * b + j, rows, :] for j in range(3)]
                for i, j in wanted:
                    term = left[i] * right[j]
                    one[i, j] = term if t == 0 else one[i, j] + term
        return sums

    first = 0
    for double, doubles in part.runs:

        def off_diagonal(group, carry, double=double, first=first):
            def two(k):
                a, *seconds = double(group * 4 + k)
                return products(a, seconds, FULL)

            m = octet(two)
            across = mu * (m[0, 0] + m[1, 1] + m[2, 2])
            for i, j in FULL:
                value = both * m[i, i] + across if i == j else lam * m[i, j] + mu * m[j, i]
                start = pl.multiple_of((3 * i + j) * part.pairs + first + group * 8, 8)
                k_ref[pl.ds(start, 8), :] = value
            return carry

        lax.fori_loop(0, doubles // 4, off_diagonal, 0)
        first += 2 * doubles

    def diagonal(group, carry):
        def two(k):
            own = [jnp.minimum(group * 8 + 2 * k + n, NF - 1) for n in range(2)]
            return [products(a, [a], part.inner)[0] for a in own]

        m = octet(two)
        across = mu * (m[0, 0] + m[1, 1] + m[2, 2])
        for c, (i, j) in enumerate(part.inner):
            value = both * m[i, j] + across if i == j else both * m[i, j]
            start = pl.multiple_of(part.diagonal + c * DIAG_UP + group * 8, 8)
            k_ref[pl.ds(start, 8), :] = value
        return carry

    if part.inner:
        lax.fori_loop(0, DIAG_UP // 8, diagonal, 0)

    if part.used < part.words:
        k_ref[pl.ds(part.used, part.words - part.used), :] = jnp.zeros(
            (part.words - part.used, count), jnp.float32
        )
    k_ref[pl.ds(part.slot, 1), :] = slots


def gather_words(part, inverse, in_ref, sum_ref):
    width = in_ref.shape[0]
    base = part.slot // LANES * LANES
    tail = in_ref[:, base : base + LANES].T
    slots = tail[part.slot - base : part.slot - base + 1, :]
    wanted = (lax.broadcasted_iota(jnp.int32, (SLOTS_DEV, width), 0) + 1).astype(jnp.float32)
    placing = (slots == wanted).astype(jnp.bfloat16)
    for tile in range(part.words // LANES):
        words = slice(tile * LANES, (tile + 1) * LANES)
        summed = pick(placing, in_ref[:, words], ((1,), (0,)))
        sum_ref[words, :] = (summed * inverse).T


def relay_kernel(plane, capacity, *refs):
    planes = len(refs) - plane
    in_refs, out_refs = refs[:planes], refs[planes:]
    for l, out_ref in enumerate(out_refs):
        for k, in_ref in enumerate(in_refs):
            out_ref[k * capacity : (k + 1) * capacity] = in_ref[l * capacity : (l + 1) * capacity]


def unfold(part, ref, whole_ref, after=lambda a: None):
    entries = {}
    for p, (a, b) in enumerate(part.blocks):
        for i, j in FULL:
            word = (3 * i + j) * part.pairs + p
            entries.setdefault(3 * a + i, {})[3 * b + j] = word
            entries.setdefault(3 * b + j, {})[3 * a + i] = word
    for c, (i, j) in enumerate(part.inner):
        for a in range(NF):
            word = part.diagonal + c * DIAG_UP + a
            entries[3 * a + i][3 * a + j] = entries[3 * a + j][3 * a + i] = word
    for m in range(NDOF):
        for n, word in sorted(entries[m].items()):
            whole_ref[m, n, :] = ref[word, :]
        if m % 3 == 2:
            after(m // 3)


def lead_owners(capacity, elements, *refs):
    in_refs, (whole_ref, inverse_ref, all_ref, sum_ref) = refs[:-4], refs[-4:]
    rows = in_refs[0].shape[0]
    for l, in_ref in enumerate(in_refs):
        all_ref[l * rows : (l + 1) * rows] = in_ref[...]
    total = jnp.sum(all_ref[:, LEAD.trace : LEAD.trace + 1]) / capacity
    inverse = 1.0 / jnp.broadcast_to(total / (NDOF * elements), (SLOTS_DEV, LANES))
    inverse_ref[...] = inverse
    gather_words(LEAD, inverse, all_ref, sum_ref)
    unfold(LEAD, sum_ref, whole_ref)


def rest_owners(in_ref, inverse_ref, whole_in, out_ref, whole_ref, sum_ref, sems):
    del whole_in
    gather_words(REST, inverse_ref[...], in_ref, sum_ref)

    def copy(stripe):
        rows = pl.ds(stripe * (NDOF // STRIPES), NDOF // STRIPES)
        return pltpu.make_async_copy(whole_ref.at[rows], out_ref.at[rows], sems.at[stripe])

    def after(a):
        if (a + 1) * STRIPES % NF == 0:
            copy((a + 1) * STRIPES // NF - 1).start()

    unfold(REST, sum_ref, whole_ref, after)
    for stripe in range(STRIPES):
        copy(stripe).wait()


def planes_of(nrow):
    most = nrow & -nrow
    return max(1, most // 2)


def shards(grads, weights, counts, lame_first, shear, dest_owner, dest_slot):
    points, _, _, count = grads.shape
    nrow, ncol = lax.axis_size("row"), lax.axis_size("col")
    ndevices = nrow * ncol
    capacity = max(2, 2 * count // ndevices)
    width = ndevices * capacity
    planes = planes_of(nrow)
    plane = ndevices // planes
    f32 = lambda *shape: jax.ShapeDtypeStruct(shape, jnp.float32)
    line = lambda v: v.reshape(1, count)
    params = pltpu.CompilerParams(vmem_limit_bytes=20 * 2**20)
    vmem = pltpu.VMEM
    hbm = pl.BlockSpec(memory_space=pltpu.MemorySpace.HBM)
    large = (NDOF, points + 8, count)

    near = lambda d, k: (d // plane ^ k) * plane + d % plane
    beside = lambda d, l: d // plane * plane + (d + l) % plane
    cost = lambda part: pl.CostEstimate(
        flops=60000 * part.words, bytes_accessed=4000000, transcendentals=0
    )
    *blocks, place, g, wg, lines = pl.pallas_call(
        functools.partial(lead_elements, plane, ndevices, capacity),
        in_specs=[hbm] * 7,
        out_shape=[f32(plane * capacity, LEAD.words)] * planes
        + [jax.ShapeDtypeStruct((1, count), jnp.int32), f32(*large), f32(*large), f32(8, count)],
        scratch_shapes=[
            vmem((points, count), jnp.float32),
            vmem((1, count), jnp.int32),
            vmem((1, count), jnp.float32),
            vmem((1, count), jnp.float32),
            vmem((1, count), jnp.int32),
            vmem((1, count), jnp.int32),
            vmem((LEAD.words, count), jnp.float32),
            pltpu.SemaphoreType.DMA((6 + STRIPES,)),
        ],
        compiler_params=params,
        cost_estimate=cost(LEAD),
        name="elements_lead",
    )(
        *(
            pltpu.with_memory_space_constraint(v, pltpu.MemorySpace.HBM)
            for v in (
                jnp.transpose(grads, (1, 2, 0, 3)).reshape(NDOF, points, count),
                weights,
                line(counts),
                line(lame_first),
                line(shear),
                line(dest_slot),
                line(dest_owner),
            )
        )
    )
    for k in HOPS(planes):
        pairs = [(d, near(d, k)) for d in range(ndevices)]
        blocks[k] = lax.ppermute(blocks[k], AXES, pairs)
    rest = pl.pallas_call(
        rest_elements,
        out_shape=f32(width, REST.words),
        out_specs=pl.BlockSpec(memory_space=pl.ANY),
        scratch_shapes=[
            vmem((REST.words, count), jnp.float32),
            vmem((width, REST.words), jnp.float32),
            pltpu.SemaphoreType.DMA((-(-REST.words // (2 * LANES)),)),
        ],
        compiler_params=params,
        cost_estimate=cost(REST),
        name="elements_rest",
    )(g, wg, lines, place)
    rest = lax.all_to_all(
        rest.reshape(ndevices, capacity, REST.words),
        AXES,
        split_axis=0,
        concat_axis=0,
        tiled=True,
    ).reshape(width, REST.words)
    blocks = pl.pallas_call(
        functools.partial(relay_kernel, plane, capacity),
        out_shape=[f32(planes * capacity, LEAD.words)] * plane,
        compiler_params=params,
        name="relay",
    )(*blocks)
    blocks = list(blocks)
    for l in range(1, plane):
        pairs = [(d, beside(d, l)) for d in range(ndevices)]
        blocks[l] = lax.ppermute(blocks[l], AXES, pairs)
    whole = f32(NDOF, NDOF, SLOTS_DEV)
    lead, inverse = pl.pallas_call(
        functools.partial(lead_owners, capacity, count * ndevices),
        out_shape=[whole, f32(SLOTS_DEV, LANES)],
        scratch_shapes=[
            vmem((width, LEAD.words), jnp.float32),
            vmem((LEAD.words, SLOTS_DEV), jnp.float32),
        ],
        compiler_params=params,
        name="owners_lead",
    )(*blocks)
    return pl.pallas_call(
        rest_owners,
        out_shape=[whole, whole],
        out_specs=[pl.BlockSpec(memory_space=pl.ANY), pl.BlockSpec(memory_space=pltpu.VMEM)],
        input_output_aliases={2: 1},
        scratch_shapes=[
            vmem((REST.words, SLOTS_DEV), jnp.float32),
            pltpu.SemaphoreType.DMA((STRIPES,)),
        ],
        compiler_params=params,
        name="owners_rest",
    )(rest, inverse, lead)[0]


def solution(mesh):
    in_specs = (
        P(None, None, None, AXES),
        P(None, AXES),
        P(AXES),
        P(AXES),
        P(AXES),
        P(AXES, None),
        P(AXES),
    )
    out_specs = P(None, None, AXES)

    return jax.shard_map(shards, mesh=mesh, in_specs=in_specs, out_specs=out_specs, check_vma=False)
```
